128 devices in a mesh: member: 2 (over y_hi), band: 64 (over x, z, y_lo, core).
Axes of the slice: x: 4, y: 4 (y_hi: 2, y_lo: 2; y = y_hi * 2 + y_lo), z: 4, core: 2. Of those that a mesh axis runs over, the one named last changes fastest.
Arguments:
- fields: bfloat16 [4, 32768, 1024], P('member', 'band'), may hold values from -17.5 to 17.5
- w_qkv: bfloat16 [1024, 3072], replicated, may hold values from -0.1875 to 0.1875
- w_out: bfloat16 [1024, 1024], replicated, may hold values from -0.1875 to 0.1875
- decoder_weight: bfloat16 [96, 1024], replicated, may hold values from -0.1875 to 0.1875
- window_reach: int32 [16], replicated, may hold values from 1 to 128
- truth: float32 [96, 32768], P(None, 'band'), may hold values from -6 to 6
- radii: int32 [3], replicated, may hold values from 1 to 16
Outputs:
- mean_score: float32 [], replicated
- decoder_grad: float32 [96, 1024], replicated
- hidden_grad: bfloat16 [4, 32768, 1024], P('member', 'band')
The draws below stay inside these ranges and needn't reach their ends.
All inputs are finite; a program needn't handle non-finite values.
Results may differ from the reference program's by a relative error of at most 0.012.
The reference program's roundings to bfloat16 on the way count: a program that leaves them out, or rounds other values in their place, can miss the bound.
Values may be sent and summed in bfloat16 or wider, within the bound.
A program may use at most 192 MiB of HBM per device.

```python
import math
import jax
import jax.numpy as jnp
from jax import lax

D = 1024
HEADS = 16
CHANNELS = 96
TOK_DEV = 512
WIN = 128
SCALES = 3
RMAX = 16
MEMBERS = 4
TOKENS = 32768


def draw_fields(key, part):
    dims_all = (MEMBERS, TOKENS, D)
    key_base = jax.random.fold_in(key, 0)
    values = jnp.clip(jax.random.normal(key_base, dims_all, jnp.float32), -6.0, 6.0)
    return values.astype(jnp.bfloat16)


def with_ends(drawn, key, low, high):
    extent = drawn.shape
    place = [jax.random.randint(jax.random.fold_in(key, axis), (), 0, extent[axis]) for axis in range(len(extent))]
    drawn = drawn.at[tuple(place)].set(low)
    longest = extent.index(max(extent))
    place[longest] = (place[longest] + 1) % extent[longest]
    return drawn.at[tuple(place)].set(high)


def shard_levels(rng, shape, shards, least, largest):
    gain = 1.0
    for dim, shards_of in shards:
        draws = jax.random.uniform(jax.random.fold_in(jax.random.fold_in(rng, 6), dim), (shards_of,), jnp.float32, least / len(shards), largest / len(shards))
        gain = gain * jnp.repeat(jnp.exp(draws), shape[dim] // shards_of).reshape((-1,) + (1,) * (len(shape) - 1 - dim))
    return gain


def gaussian(stream_key, shape, scale, reach, pieces=(), held_as=jnp.bfloat16):
    factor_of = shard_levels(stream_key, shape, pieces, -0.22, 0.18) if pieces else 1.0
    drawn = jax.random.normal(stream_key, shape, jnp.float32) * scale * factor_of
    return jnp.minimum(jnp.maximum(drawn, -reach), reach).astype(held_as)


def setup_inputs(seed: int = 0) -> dict:
    keys = jax.random.split(jax.random.key(seed), 8)
    fields = draw_fields(jax.random.fold_in(keys[7], 71), 0)
    w_qkv = gaussian(keys[1], (D, 3 * D), D ** -0.5, 0.1875)
    w_out = gaussian(keys[2], (D, D), D ** -0.5, 0.1875)
    decoder_weight = gaussian(keys[3], (CHANNELS, D), D ** -0.5, 0.1875)
    window_reach = with_ends(jax.random.randint(keys[4], (HEADS,), 1, WIN + 1), jax.random.fold_in(keys[4], 1), 1, WIN).astype(jnp.int32)
    truth = gaussian(keys[5], (CHANNELS, TOKENS), 1.0, 6.0, ((1, 64),), jnp.float32)
    radii = jax.random.randint(keys[6], (SCALES,), 1, RMAX + 1).astype(jnp.int32)
    return dict(fields=fields, w_qkv=w_qkv, w_out=w_out, decoder_weight=decoder_weight, window_reach=window_reach, truth=truth, radii=radii)


softness = 0.1

def kernel_table(radii):
    offsets = jnp.arange(-RMAX, RMAX + 1).astype(jnp.float32)
    reaches = radii.astype(jnp.float32)[:, None]
    spread_width = 0.5 * reaches
    weights_raw = jnp.exp(-(offsets[None, :] * offsets[None, :]) / (2.0 * spread_width * spread_width))
    weights_raw = jnp.where(jnp.abs(offsets)[None, :] <= reaches, weights_raw, 0.0)
    return weights_raw / lax.optimization_barrier(jnp.sum(weights_raw, axis=1, keepdims=True))

def filter_rows(padded, kernel, sequence_length):
    shaped = (kernel.shape[0],) + (1,) * (padded.ndim - 1)
    result = jnp.zeros((kernel.shape[0],) + padded.shape[1:-1] + (sequence_length,), jnp.float32)
    for position in range(kernel.shape[1]):
        result = result + kernel[:, position].reshape(shaped) * padded[..., position:position + sequence_length]
    return result

def soft_abs(values):
    return jnp.sqrt(values * values + softness * softness)

def fair_score(ensemble, observed):
    members_total = ensemble.shape[1]
    skill_term = jnp.zeros(observed.shape, jnp.float32)
    spread_term = jnp.zeros(observed.shape, jnp.float32)
    slopes = []
    for member_a in range(members_total):
        difference = ensemble[:, member_a] - observed
        magnitude = soft_abs(difference)
        skill_term = skill_term + magnitude
        slopes.append(difference / magnitude / members_total)
    pair_weight = 1.0 / (members_total * (members_total - 1))
    for member_a in range(members_total):
        for member_b in range(member_a + 1, members_total):
            difference = ensemble[:, member_a] - ensemble[:, member_b]
            magnitude = soft_abs(difference)
            spread_term = spread_term + magnitude
            slopes[member_a] = slopes[member_a] - pair_weight * difference / magnitude
            slopes[member_b] = slopes[member_b] + pair_weight * difference / magnitude
    scores = skill_term / members_total - pair_weight * spread_term
    return (scores, jnp.stack(slopes, axis=1))

def attend_member(member_fields, w_qkv, w_out, window_reach):
    tokens_total, width = member_fields.shape
    head_count = window_reach.shape[0]
    head_size = width // head_count
    packed = jnp.dot(member_fields, w_qkv, preferred_element_type=jnp.float32).astype(jnp.bfloat16)
    queries = packed[:, :width]
    key_pad = jnp.pad(packed[:, width:2 * width], ((WIN, WIN), (0, 0)))
    value_pad = jnp.pad(packed[:, 2 * width:], ((WIN, WIN), (0, 0)))
    key_count = TOK_DEV + 2 * WIN

    def one_block(block):
        start = (block * TOK_DEV).astype(jnp.int32)
        block_q = lax.dynamic_slice_in_dim(queries, start, TOK_DEV, 0).reshape(TOK_DEV, head_count, head_size).astype(jnp.float32)
        block_k = lax.dynamic_slice_in_dim(key_pad, start, key_count, 0).reshape(key_count, head_count, head_size).astype(jnp.float32)
        block_v = lax.dynamic_slice_in_dim(value_pad, start, key_count, 0).reshape(key_count, head_count, head_size).astype(jnp.float32)
        logits = jnp.einsum('qhd,khd->hqk', block_q, block_k) * head_size ** (-0.5)
        query_pos = start + jnp.arange(TOK_DEV, dtype=jnp.int32)
        key_pos = start - WIN + jnp.arange(key_count, dtype=jnp.int32)
        offset = key_pos[None, :] - query_pos[:, None]
        inside = (key_pos >= 0) & (key_pos < tokens_total)
        allowed = (jnp.abs(offset)[None] <= window_reach[:, None, None]) & inside[None, None, :]
        logits = jnp.where(allowed, logits, -1e+30)
        peak = lax.optimization_barrier(jnp.max(logits, axis=2, keepdims=True))
        expo = jnp.exp(logits - peak)
        probs = (expo / lax.optimization_barrier(jnp.sum(expo, axis=2, keepdims=True))).astype(jnp.bfloat16)
        mixed = jnp.einsum('hqk,khd->qhd', probs.astype(jnp.float32), block_v).astype(jnp.bfloat16)
        return mixed.reshape(TOK_DEV, width)
    attended = lax.map(one_block, jnp.arange(tokens_total // TOK_DEV, dtype=jnp.int32)).reshape(tokens_total, width)
    mixed_out = jnp.dot(attended, w_out, preferred_element_type=jnp.float32) + member_fields.astype(jnp.float32)
    return mixed_out.astype(jnp.bfloat16)

def reference(fields, w_qkv, w_out, decoder_weight, window_reach, truth, radii):
    hidden_state = jnp.stack([attend_member(fields[member_index], w_qkv, w_out, window_reach) for member_index in range(MEMBERS)])
    predicted_fields = jnp.einsum('ly,pey->ple', decoder_weight.astype(jnp.float32), hidden_state.astype(jnp.float32))
    kernel = kernel_table(radii)
    sequence_length = predicted_fields.shape[2]
    stacked_scales = jnp.concatenate([predicted_fields, truth.astype(jnp.float32)[None]], axis=0)
    padded = jnp.pad(stacked_scales, ((0, 0), (0, 0), (RMAX, RMAX)))
    smoothed = filter_rows(padded[None], kernel, sequence_length)
    scores, slopes = fair_score(smoothed[:, :MEMBERS], smoothed[:, MEMBERS])
    adjoint = filter_rows(jnp.pad(slopes, ((0, 0), (0, 0), (0, 0), (RMAX, RMAX))), kernel, sequence_length)
    cotangent = lax.optimization_barrier(jnp.sum(adjoint, axis=0)).astype(jnp.bfloat16)
    hidden_grad = jnp.einsum('mct,cd->mtd', cotangent.astype(jnp.float32), decoder_weight.astype(jnp.float32)).astype(jnp.bfloat16)
    decoder_grad = jnp.einsum('mct,mtd->cd', cotangent.astype(jnp.float32), hidden_state.astype(jnp.float32)) / math.sqrt(MEMBERS * sequence_length)
    mean_score = jnp.sum(scores) / (SCALES * CHANNELS * sequence_length)
    return (mean_score, decoder_grad, hidden_grad)
```

```python
import math

import jax
import jax.numpy as jnp
from jax import lax
from jax.experimental import pallas as pl
from jax.experimental.pallas import tpu as pltpu
from jax.sharding import PartitionSpec as P

WIN = 128
RMAX = 16
SOFT = 0.01
LANES = 128
COLS = 256
NEG = -1e30
PAIR_UNROLL = 4
ROWS = 192
RIM = 2 * RMAX
GROUP = 16
BF = jnp.bfloat16
F32 = jnp.float32
MESH = pl.DeviceIdType.MESH


def aligned(index, step, size):
    return pl.ds(pl.multiple_of(index * step, step), size)


def front_kernel(
    reach, fields, wqkv, wout, decoder, hidden, forecast,
    own, rim, w, wo, packed, attended, offset, held, sent, load_sem, send_sem, recv_sem, out_sem,
):
    band = lax.axis_index("band")
    count = lax.axis_size("band")
    right = lax.rem(band + 1, count)
    left = lax.rem(band + count - 1, count)
    members, toks, width = fields.shape
    heads = reach.shape[0]
    scale = (width // heads) ** -0.5 * math.log2(math.e)
    total = toks * count

    loads = [
        pltpu.make_async_copy(fields.at[m], own.at[pl.ds(m * toks, toks)], load_sem.at[m])
        for m in range(members)
    ]
    weights = [
        pltpu.make_async_copy(
            wqkv.at[:, pl.ds(j * width, width)], w.at[:, pl.ds(j * width, width)],
            load_sem.at[members + j],
        )
        for j in range(3)
    ]
    last = pltpu.make_async_copy(wout, wo, load_sem.at[members + 3])
    for copy in loads + weights + [last]:
        copy.start()

    barrier = pltpu.get_barrier_semaphore()
    for neighbour in (left, right):
        pl.semaphore_signal(barrier, inc=1, device_id={"band": neighbour}, device_id_type=MESH)
    pl.semaphore_wait(barrier, 2)
    copies = []
    for m in range(members):
        for side, (start, target) in enumerate(((toks - WIN, right), (0, left))):
            slot = 2 * m + side
            copies.append(
                pltpu.make_async_remote_copy(
                    src_ref=fields.at[m, pl.ds(start, WIN)],
                    dst_ref=rim.at[pl.ds(slot * WIN, WIN)],
                    send_sem=send_sem.at[slot],
                    recv_sem=recv_sem.at[slot],
                    device_id={"band": target},
                    device_id_type=MESH,
                )
            )
    for copy in copies:
        copy.start()

    def project(n, carry):
        cols = aligned(n, COLS, COLS)
        y = jnp.dot(own[...], w[:, cols], preferred_element_type=F32).astype(BF)
        for m in range(members):
            packed[m, pl.ds(WIN, toks), cols] = y[m * toks : (m + 1) * toks]
        return carry

    for copy in loads:
        copy.wait()
    steps = width // COLS
    for j in range(3):
        weights[j].wait()
        lax.fori_loop(j * steps, (j + 1) * steps, project, 0)

    for copy in copies:
        copy.wait()

    def project_rim(n, carry):
        cols = aligned(n, COLS, COLS)
        y = jnp.dot(rim[...], w[:, cols], preferred_element_type=F32).astype(BF)
        for m in range(members):
            packed[m, pl.ds(0, WIN), cols] = y[2 * m * WIN : (2 * m + 1) * WIN]
            packed[m, pl.ds(WIN + toks, WIN), cols] = y[(2 * m + 1) * WIN : (2 * m + 2) * WIN]
        return carry

    lax.fori_loop(steps, 3 * steps, project_rim, 0)
    last.wait()

    first = lax.broadcasted_iota(jnp.int32, (WIN, LANES), 1) < LANES // 2
    low = jnp.where(first, 1.0, 0.0).astype(BF)
    high = jnp.where(first, 0.0, 1.0).astype(BF)
    ones = jnp.ones((3 * WIN, LANES), BF)

    def one_pair(m, b, p):
        queries = packed[m, aligned(b + 1, WIN, WIN), aligned(p, LANES, LANES)]
        keys = packed[m, aligned(b, WIN, 3 * WIN), aligned(p + width // LANES, LANES, LANES)]
        values = packed[m, aligned(b, WIN, 3 * WIN), aligned(p + 2 * width // LANES, LANES, LANES)]
        both = jnp.concatenate([queries * low, queries * high], axis=0)
        logits = lax.dot_general(both, keys, (((1,), (1,)), ((), ())), preferred_element_type=F32)
        away = offset[...]
        logits = jnp.concatenate(
            [
                jnp.where(away <= reach[2 * p], logits[:WIN], NEG),
                jnp.where(away <= reach[2 * p + 1], logits[WIN:], NEG),
            ],
            axis=0,
        )
        peak = jnp.max(logits, axis=1, keepdims=True)
        expo = jnp.exp2((logits - peak) * scale).astype(BF)
        mixed = jnp.dot(
            expo, jnp.concatenate([values, ones], axis=1), preferred_element_type=F32
        )
        top = jnp.where(first, mixed[:WIN, :LANES], mixed[WIN:, :LANES])
        norm = jnp.where(first, mixed[:WIN, LANES:], mixed[WIN:, LANES:])
        attended[aligned(b, WIN, WIN), aligned(p, LANES, LANES)] = (top / norm).astype(BF)

    def one_block(m, b):
        key = lax.broadcasted_iota(jnp.int32, (WIN, 3 * WIN), 1)
        query = lax.broadcasted_iota(jnp.int32, (WIN, 3 * WIN), 0)
        place = key + (band * toks + b * WIN - WIN)
        inside = (place >= 0) & (place < total)
        offset[...] = jnp.where(inside, jnp.abs(key - WIN - query), total)

        def some_pairs(i, carry):
            for u in range(PAIR_UNROLL):
                one_pair(m, b, i * PAIR_UNROLL + u)
            return carry

        lax.fori_loop(0, heads // 2 // PAIR_UNROLL, some_pairs, 0)

    def one_member(m, carry):
        def step(b, inner):
            one_block(m, b)
            return inner

        lax.fori_loop(0, toks // WIN, step, 0)
        rows = aligned(m, toks, toks)

        def mix(n, inner):
            cols = aligned(n, COLS, COLS)
            y = jnp.dot(attended[...], wo[:, cols], preferred_element_type=F32)
            held[m, :, cols] = (y + own[rows, cols].astype(F32)).astype(BF)
            return inner

        lax.fori_loop(0, steps, mix, 0)
        sent[m] = lax.dot_general(
            held[m], decoder[...], (((1,), (1,)), ((), ())), preferred_element_type=F32
        ).astype(BF)
        return carry

    lax.fori_loop(0, members, one_member, 0)
    outs = [
        pltpu.make_async_copy(held, hidden, out_sem.at[0]),
        pltpu.make_async_copy(sent, forecast, out_sem.at[1]),
    ]
    for copy in outs:
        copy.start()
    for copy in outs:
        copy.wait()


def tail_kernel(
    points, divisor, radii, forecast, hidden, truth, cot, decoder_grad, score,
    buf, taps, slopes, held, parts, got, sums, mids, final, load_sem,
    send_sem, recv_sem, send_a, recv_a, send_b, recv_b, send_c, recv_c,
):
    band = lax.axis_index("band")
    member = lax.axis_index("member")
    count = lax.axis_size("band")
    right = lax.rem(band + 1, count)
    left = lax.rem(band + count - 1, count)
    other = 1 - member
    members, toks, lanes = forecast.shape
    channels = truth.shape[0]
    width = hidden.shape[2]
    total = toks * count
    planes = count // GROUP
    plane = band // GROUP
    place = lax.rem(band, GROUP)
    base = plane * GROUP
    squad = 2 * planes
    rank = member * planes + plane

    def in_group(step):
        return lax.rem(place + step, GROUP)

    def in_squad(step):
        return lax.rem(rank + step, squad)

    def squad_device(r):
        return {"member": r // planes, "band": lax.rem(r, planes) * GROUP + place}

    load_f = pltpu.make_async_copy(forecast, buf.at[pl.ds(0, members), pl.ds(RIM, toks)], load_sem.at[0])
    load_h = pltpu.make_async_copy(hidden, held, load_sem.at[1])
    load_f.start()
    load_h.start()

    barrier = pltpu.get_barrier_semaphore()
    for m in (member, other):
        for b in (left, right):
            pl.semaphore_signal(barrier, inc=1, device_id={"member": m, "band": b}, device_id_type=MESH)
    for step in range(1, GROUP):
        pl.semaphore_signal(barrier, inc=1, device_id={"band": base + in_group(step)}, device_id_type=MESH)
    for step in range(1, squad):
        pl.semaphore_signal(barrier, inc=1, device_id=squad_device(in_squad(step)), device_id_type=MESH)

    shown = jnp.concatenate([truth[...], jnp.zeros((lanes - channels, toks), F32)], axis=0)
    buf[2 * members, pl.ds(RIM, toks), :] = shown.T.astype(BF)
    end = RIM + toks + RIM
    for st in range(2 * members + 1):
        buf[st, pl.ds(end, buf.shape[1] - end), :] = jnp.zeros((buf.shape[1] - end, lanes), BF)
    for s in range(3):
        for m in range(members):
            rows = 3 * ROWS
            slopes[s, pl.ds(rows, slopes.shape[1] - rows), pl.ds(m * lanes, lanes)] = jnp.zeros(
                (slopes.shape[1] - rows, lanes), BF
            )
    pl.semaphore_wait(barrier, 4 + GROUP - 1 + squad - 1)
    load_f.wait()

    own = pl.ds(0, members)
    theirs = pl.ds(members, members)
    observed = pl.ds(2 * members, 1)
    tail = pl.ds(toks, RIM)
    head = pl.ds(RIM, RIM)
    before = pl.ds(0, RIM)
    after = pl.ds(RIM + toks, RIM)
    body = pl.ds(RIM, toks)
    plan = [
        (own, tail, own, before, member, right),
        (own, head, own, after, member, left),
        (own, tail, theirs, before, other, right),
        (own, head, theirs, after, other, left),
        (observed, tail, observed, before, member, right),
        (observed, head, observed, after, member, left),
        (own, body, theirs, body, other, band),
    ]
    copies = [
        pltpu.make_async_remote_copy(
            src_ref=buf.at[s0, r0], dst_ref=buf.at[s1, r1],
            send_sem=send_sem.at[i], recv_sem=recv_sem.at[i],
            device_id={"member": m, "band": b}, device_id_type=MESH,
        )
        for i, (s0, r0, s1, r1, m, b) in enumerate(plan)
    ]
    for copy in copies:
        copy.start()

    span = lax.broadcasted_iota(jnp.int32, (8, lanes), 1) - RMAX
    apart = (
        lax.broadcasted_iota(jnp.int32, (ROWS, COLS), 1)
        - lax.broadcasted_iota(jnp.int32, (ROWS, COLS), 0)
        - RMAX
    )
    for s in range(3):
        radius = jnp.full((8, lanes), radii[s], jnp.int32).astype(F32)
        rate = 2.0 / (radius * radius)
        near = span.astype(F32)
        line = jnp.where(jnp.abs(span) <= radii[s], jnp.exp(-(near * near) * rate), 0.0)
        inverse = 1.0 / jnp.sum(line, axis=1, keepdims=True)
        far = apart.astype(F32)
        table = jnp.exp(-(far * far) * jnp.broadcast_to(rate[:1, :1], (ROWS, COLS)))
        table = jnp.where(jnp.abs(apart) <= radii[s], table, 0.0)
        table = table * jnp.broadcast_to(inverse[:1], (ROWS, COLS))
        taps[pl.ds(s * ROWS, ROWS), :] = table.astype(BF)

    for copy in copies:
        copy.wait()
    for st in range(2 * members + 1):
        for rows, keep in ((before, band > 0), (after, band < count - 1)):
            value = buf[st, rows, :].astype(F32)
            flag = jnp.full((RIM, lanes), keep.astype(jnp.int32), jnp.int32)
            buf[st, rows, :] = jnp.where(flag > 0, value, 0.0).astype(BF)

    line = lax.broadcasted_iota(jnp.int32, (ROWS, lanes), 0)
    lane = lax.broadcasted_iota(jnp.int32, (ROWS, lanes), 1)

    def contrast(a, b):
        z = a - b
        square = z * z + SOFT
        inverse = lax.rsqrt(square)
        return z * inverse, square * inverse

    def score_block(b, acc):
        window = aligned(b, ROWS, COLS)
        point = line + (b * ROWS - RMAX)
        counted = (point >= 0) & (point < toks) & (lane < channels)
        globe = point + band * toks
        inside = (globe >= 0) & (globe < total)
        streams = jnp.concatenate([buf[st, window, :] for st in range(2 * members + 1)], axis=1)
        for s in range(3):
            x = jnp.dot(taps[pl.ds(s * ROWS, ROWS), :], streams, preferred_element_type=F32)
            a0, a1, b0, b1, y = [x[:, i * lanes : (i + 1) * lanes] for i in range(5)]
            g0, h0 = contrast(a0, y)
            g1, h1 = contrast(a1, y)
            g01, h01 = contrast(a0, a1)
            g02, h02 = contrast(a0, b0)
            g03, h03 = contrast(a0, b1)
            g12, h12 = contrast(a1, b0)
            g13, h13 = contrast(a1, b1)
            s0 = 0.25 * g0 - (g01 + g02 + g03) * (1.0 / 12.0)
            s1 = 0.25 * g1 - (g12 + g13 - g01) * (1.0 / 12.0)
            slopes[s, aligned(b, ROWS, ROWS), pl.ds(0, lanes)] = jnp.where(inside, s0, 0.0).astype(BF)
            slopes[s, aligned(b, ROWS, ROWS), pl.ds(lanes, lanes)] = jnp.where(inside, s1, 0.0).astype(BF)
            value = 0.25 * (h0 + h1) - h01 * (1.0 / 12.0) - (h02 + h03 + h12 + h13) * (1.0 / 24.0)
            acc = acc + jnp.sum(jnp.where(counted, value, 0.0), axis=0, keepdims=True)
        return acc

    acc = lax.fori_loop(0, 3, score_block, jnp.zeros((1, lanes), F32))

    for b in range(3):
        rows = min(ROWS, toks - b * ROWS)
        c = jnp.zeros((ROWS, 2 * lanes), F32)
        for s in range(3):
            c = c + jnp.dot(
                taps[pl.ds(s * ROWS, ROWS), :], slopes[s, pl.ds(b * ROWS, COLS), :],
                preferred_element_type=F32,
            )
        for m in range(members):
            cot[m, pl.ds(b * ROWS, rows), :] = c[:rows, m * lanes : (m + 1) * lanes].astype(BF)

    load_h.wait()
    half = channels // 2
    narrow = width // LANES
    at = lax.broadcasted_iota(jnp.int32, (16, lanes), 0)
    upper = acc.astype(BF).astype(F32)
    extra = jnp.where(at == 0, upper, jnp.where(at == 1, acc - upper, 0.0)).astype(BF)
    for j in range(width // COLS):
        cols = pl.ds(j * COLS, COLS)
        y = jnp.zeros((lanes, COLS), F32)
        for m in range(members):
            y = y + lax.dot_general(
                cot[m], held[m, :, cols], (((0,), (0,)), ((), ())), preferred_element_type=F32
            )
        y = y.astype(BF)
        for i in range(COLS // LANES):
            for h in range(2):
                g = h * narrow + j * (COLS // LANES) + i
                parts[g, pl.ds(0, half), :] = y[h * half : (h + 1) * half, i * LANES : (i + 1) * LANES]
                parts[g, pl.ds(half, 16), :] = extra

    def copy_a(step):
        g = in_group(step)
        return pltpu.make_async_remote_copy(
            src_ref=parts.at[g], dst_ref=got.at[place], send_sem=send_a.at[step],
            recv_sem=recv_a.at[place], device_id={"band": base + g}, device_id_type=MESH,
        )

    def arrived_a(step):
        g = in_group(step)
        return pltpu.make_async_remote_copy(
            src_ref=parts.at[g], dst_ref=got.at[g], send_sem=send_a.at[step],
            recv_sem=recv_a.at[g], device_id={"band": base + g}, device_id_type=MESH,
        )

    for step in range(1, GROUP):
        copy_a(step).start()
    got[place] = parts[place]
    for step in range(1, GROUP):
        arrived_a(step).wait()
    piece = got[0].astype(F32)
    for g in range(1, GROUP):
        piece = piece + got[g].astype(F32)
    sums[...] = piece
    mids[rank] = piece

    def copy_b(step):
        r = in_squad(step)
        return pltpu.make_async_remote_copy(
            src_ref=sums, dst_ref=mids.at[rank], send_sem=send_b.at[step],
            recv_sem=recv_b.at[rank], device_id=squad_device(r), device_id_type=MESH,
        )

    def arrived_b(step):
        r = in_squad(step)
        return pltpu.make_async_remote_copy(
            src_ref=sums, dst_ref=mids.at[r], send_sem=send_b.at[step],
            recv_sem=recv_b.at[r], device_id=squad_device(r), device_id_type=MESH,
        )

    for step in range(1, squad):
        copy_b(step).start()
    for step in range(1, squad):
        arrived_b(step).wait()
    piece = mids[0]
    for r in range(1, squad):
        piece = piece + mids[r]
    final[place] = (piece[:half] * (1.0 / divisor)).astype(BF)

    def copy_c(step):
        g = in_group(step)
        return pltpu.make_async_remote_copy(
            src_ref=final.at[place], dst_ref=final.at[place], send_sem=send_c.at[step],
            recv_sem=recv_c.at[place], device_id={"band": base + g}, device_id_type=MESH,
        )

    def arrived_c(step):
        g = in_group(step)
        return pltpu.make_async_remote_copy(
            src_ref=final.at[place], dst_ref=final.at[g], send_sem=send_c.at[step],
            recv_sem=recv_c.at[g], device_id={"band": base + g}, device_id_type=MESH,
        )

    for step in range(1, GROUP):
        copy_c(step).start()
    whole = jnp.sum(piece[half : half + 1] + piece[half + 1 : half + 2], axis=1, keepdims=True)
    score[...] = jnp.broadcast_to(whole * (1.0 / points), (8, lanes))
    for step in range(1, GROUP):
        arrived_c(step).wait()
    for g in range(GROUP):
        h, j = g // narrow, g % narrow
        decoder_grad[pl.ds(h * half, half), pl.ds(j * LANES, LANES)] = final[g].astype(F32)


VM = pl.BlockSpec(memory_space=pltpu.VMEM)
SM = pl.BlockSpec(memory_space=pltpu.SMEM)
ANY = pl.BlockSpec(memory_space=pl.ANY)
DMA = pltpu.SemaphoreType.DMA


def front(fields, w_qkv, w_out, decoder, window_reach):
    members, toks, width = fields.shape
    return pl.pallas_call(
        front_kernel,
        out_shape=(
            jax.ShapeDtypeStruct((members, toks, width), BF),
            jax.ShapeDtypeStruct((members, toks, LANES), BF),
        ),
        in_specs=[SM, ANY, ANY, ANY, VM],
        out_specs=(ANY, ANY),
        scratch_shapes=[
            pltpu.VMEM((members * toks, width), BF),
            pltpu.VMEM((members * 2 * WIN, width), BF),
            pltpu.VMEM((width, 3 * width), BF),
            pltpu.VMEM((width, width), BF),
            pltpu.VMEM((members, toks + 2 * WIN, 3 * width), BF),
            pltpu.VMEM((toks, width), BF),
            pltpu.VMEM((WIN, 3 * WIN), jnp.int32),
            pltpu.VMEM((members, toks, width), BF),
            pltpu.VMEM((members, toks, LANES), BF),
            DMA((members + 4,)),
            DMA((2 * members,)),
            DMA((2 * members,)),
            DMA((2,)),
        ],
        compiler_params=pltpu.CompilerParams(
            collective_id=0, has_side_effects=True, vmem_limit_bytes=60 << 20
        ),
    )(window_reach, fields, w_qkv, w_out, decoder)


def tail(forecast, hidden, truth, radii, points, divisor, squad):
    members, toks, width = hidden.shape
    channels = truth.shape[0]
    long = 2 * ROWS + COLS
    return pl.pallas_call(
        lambda *refs: tail_kernel(points, divisor, *refs),
        out_shape=(
            jax.ShapeDtypeStruct((members, toks, LANES), BF),
            jax.ShapeDtypeStruct((channels, width), F32),
            jax.ShapeDtypeStruct((8, LANES), F32),
        ),
        in_specs=[SM, ANY, ANY, VM],
        out_specs=(VM, VM, VM),
        scratch_shapes=[
            pltpu.VMEM((2 * members + 1, long, LANES), BF),
            pltpu.VMEM((3 * ROWS, COLS), BF),
            pltpu.VMEM((3, long, members * LANES), BF),
            pltpu.VMEM((members, toks, width), BF),
            pltpu.VMEM((GROUP, channels // 2 + 16, LANES), BF),
            pltpu.VMEM((GROUP, channels // 2 + 16, LANES), BF),
            pltpu.VMEM((channels // 2 + 16, LANES), F32),
            pltpu.VMEM((squad, channels // 2 + 16, LANES), F32),
            pltpu.VMEM((GROUP, channels // 2, LANES), BF),
            DMA((2,)),
            DMA((7,)),
            DMA((7,)),
            DMA((GROUP,)),
            DMA((GROUP,)),
            DMA((squad,)),
            DMA((squad,)),
            DMA((GROUP,)),
            DMA((GROUP,)),
        ],
        compiler_params=pltpu.CompilerParams(
            collective_id=1, has_side_effects=True, vmem_limit_bytes=60 << 20
        ),
    )(radii, forecast, hidden, truth)


def local(fields, w_qkv, w_out, decoder_weight, window_reach, truth, radii):
    members_here, tokens_here, width = fields.shape
    channels = decoder_weight.shape[0]
    count = lax.axis_size("band")
    tokens_total = tokens_here * count
    members_total = members_here * lax.axis_size("member")
    decoder = jnp.pad(decoder_weight, ((0, LANES - channels), (0, 0)))
    hidden, forecast = front(fields, w_qkv, w_out, decoder, window_reach)
    points = radii.shape[0] * channels * tokens_total
    divisor = math.sqrt(members_total * tokens_total)
    squad = lax.axis_size("member") * (count // GROUP)
    cot, decoder_grad, score = tail(forecast, hidden, truth, radii, points, divisor, squad)
    hidden_grad = jnp.einsum(
        "mtc,cd->mtd", cot, decoder, preferred_element_type=jnp.float32
    ).astype(jnp.bfloat16)
    return (score[0, 0], decoder_grad, hidden_grad)


def solution(mesh):
    placed = (P("member", "band", None), P(), P(), P(), P(), P(None, "band"), P())
    return jax.shard_map(
        local,
        mesh=mesh,
        in_specs=placed,
        out_specs=(P(), P(), P("member", "band", None)),
        check_vma=False,
    )
```
